768 devices in a mesh: ta: 48 (over y, z_lo, core), gz: 16 (over x, z_hi).
Axes of the slice: x: 4, y: 8, z: 12 (z_hi: 4, z_lo: 3; z = z_hi * 3 + z_lo), core: 2. Of those that a mesh axis runs over, the one named last changes fastest.
Arguments:
- source: bfloat16 [48, 16, 2, 4, 3, 12, 256], P('ta', 'gz'), may hold values from -6 to 6
- gauge_field: bfloat16 [48, 16, 4, 2, 3, 3, 256], P('ta', 'gz'), may hold values from -2.5 to 2.5
Outputs:
- twice_applied: bfloat16 [48, 16, 2, 4, 3, 12, 256], P('ta', 'gz')
The draws below stay inside these ranges and needn't reach their ends.
All inputs are finite; a program needn't handle non-finite values.
Results may differ from the reference program's by a relative error of at most 0.0075.
Values may be sent and summed in bfloat16 or wider, within the bound.
No kernel may reach another device: no remote copies, remote signals or barrier semaphores. Data moves between devices by JAX's collectives and lax.ppermute only.
A program may use at most 64 MiB of HBM per device.

```python
import jax
import jax.numpy as jnp
from jax import lax

SPINS = 4
COLORS = 3
RHS = 12
NY = 16
NX = 16
NT = 48
NZ = 16
SITES = 256


def steps_of(stream_key, extent, pieces, least, largest):
    factor_of, own = 1.0, jax.random.fold_in(stream_key, 6)
    for axis_at, parts in pieces:
        steps = jnp.exp(jax.random.uniform(jax.random.fold_in(own, axis_at), (parts,), jnp.float32, least / len(pieces), largest / len(pieces)))
        factor_of = factor_of * jnp.repeat(steps, extent[axis_at] // parts).reshape([-1 if axis == axis_at else 1 for axis in range(len(extent))])
    return factor_of


def gaussian(key, dims, spread, reach, pieces=(), kind=jnp.bfloat16):
    gain = steps_of(key, dims, pieces, -0.22, 0.18) if pieces else 1.0
    array = jax.random.normal(key, dims, jnp.float32) * spread * gain
    return jnp.minimum(jnp.maximum(array, -reach), reach).astype(kind)


def setup_inputs(seed: int = 0) -> dict:
    seeds = jax.random.split(jax.random.key(seed), 3)
    source = gaussian(seeds[0], (NT, NZ, 2, SPINS, COLORS, RHS, SITES), 1.0, 6.0, ((0, 48), (1, 16)))
    gauge_field = gaussian(seeds[1], (NT, NZ, 4, 2, COLORS, COLORS, SITES), 0.4, 2.5, ((0, 48), (1, 16)))
    return dict(source=source, gauge_field=gauge_field)


HOPPING = 0.124
GAMMA_PERM = ((3, 2, 1, 0), (3, 2, 1, 0), (2, 3, 0, 1), (2, 3, 0, 1))
GAMMA_PHASE = (((0, 1), (0, 1), (0, -1), (0, -1)),
               ((-1, 0), (1, 0), (1, 0), (-1, 0)),
               ((0, 1), (0, -1), (0, -1), (0, 1)),
               ((1, 0), (1, 0), (1, 0), (1, 0)))


def project(spinor, direction, hop_sign):
    real_part = spinor[..., 0, :, :, :, :].astype(jnp.float32)
    imag_part = spinor[..., 1, :, :, :, :].astype(jnp.float32)
    upper_real = []
    upper_imag = []
    for spin_row in range(2):
        partner = GAMMA_PERM[direction][spin_row]
        phase_re, phase_im = GAMMA_PHASE[direction][spin_row]
        mixed_re = phase_re * real_part[..., partner, :, :, :] - phase_im * imag_part[..., partner, :, :, :]
        mixed_im = phase_re * imag_part[..., partner, :, :, :] + phase_im * real_part[..., partner, :, :, :]
        upper_real.append(real_part[..., spin_row, :, :, :] - hop_sign * mixed_re)
        upper_imag.append(imag_part[..., spin_row, :, :, :] - hop_sign * mixed_im)
    stacked = jnp.stack([jnp.stack(upper_real, -4), jnp.stack(upper_imag, -4)], -5)
    return stacked.astype(jnp.bfloat16)


def color_product(link_field, half_spin, adjoint):
    link_re = link_field[..., 0, :, :, :].astype(jnp.float32)
    link_im = link_field[..., 1, :, :, :].astype(jnp.float32)
    if adjoint:
        link_re = jnp.swapaxes(link_re, -3, -2)
        link_im = -jnp.swapaxes(link_im, -3, -2)
    half_re = half_spin[..., 0, :, :, :, :].astype(jnp.float32)
    half_im = half_spin[..., 1, :, :, :, :].astype(jnp.float32)
    total_re = None
    total_im = None
    for column in range(3):
        mat_re = link_re[..., None, :, column, None, :]
        mat_im = link_im[..., None, :, column, None, :]
        vec_re = half_re[..., :, None, column, :, :]
        vec_im = half_im[..., :, None, column, :, :]
        term_re = mat_re * vec_re - mat_im * vec_im
        term_im = mat_re * vec_im + mat_im * vec_re
        total_re = term_re if total_re is None else total_re + term_re
        total_im = term_im if total_im is None else total_im + term_im
    return jnp.stack([total_re, total_im], -5)


def rebuild(product, direction, hop_sign):
    prod_re = product[..., 0, :, :, :, :]
    prod_im = product[..., 1, :, :, :, :]
    rows_re = [prod_re[..., 0, :, :, :], prod_re[..., 1, :, :, :]]
    rows_im = [prod_im[..., 0, :, :, :], prod_im[..., 1, :, :, :]]
    for spin_row in (2, 3):
        partner = GAMMA_PERM[direction][spin_row]
        phase_re, phase_im = GAMMA_PHASE[direction][spin_row]
        rows_re.append(-hop_sign * (phase_re * prod_re[..., partner, :, :, :] - phase_im * prod_im[..., partner, :, :, :]))
        rows_im.append(-hop_sign * (phase_re * prod_im[..., partner, :, :, :] + phase_im * prod_re[..., partner, :, :, :]))
    return jnp.stack([jnp.stack(rows_re, -4), jnp.stack(rows_im, -4)], -5)


def space_roll(values, direction, amount):
    full_shape = values.shape
    plane_grid = values.reshape(full_shape[:-1] + (NY, NX))
    rolled = jnp.roll(plane_grid, amount, axis=(-1 if direction == 0 else -2))
    return rolled.reshape(full_shape)


def space_hops(spinor, link_all):
    hop_sum = None
    for direction in (0, 1):
        link_field = link_all[..., direction, :, :, :, :]
        ahead_half = space_roll(project(spinor, direction, 1), direction, -1)
        term = rebuild(color_product(link_field, ahead_half, False), direction, 1)
        hop_sum = term if hop_sum is None else hop_sum + term
        behind = color_product(link_field, project(spinor, direction, -1), True)
        hop_sum = hop_sum + rebuild(space_roll(behind, direction, 1), direction, -1)
    return hop_sum


def apply_all(spinor, gauge_field):
    time_count = spinor.shape[0]

    def one_slice(slice_index):
        before_index = (slice_index - 1) % time_count
        after_index = (slice_index + 1) % time_count
        current = spinor[slice_index]
        links_now = gauge_field[slice_index]
        hop_sum = space_hops(current, links_now)
        ahead_half = jnp.roll(project(current, 2, 1), -1, axis=0)
        hop_sum = hop_sum + rebuild(color_product(links_now[:, 2], ahead_half, False), 2, 1)
        behind = jnp.roll(color_product(links_now[:, 2], project(current, 2, -1), True), 1, axis=0)
        hop_sum = hop_sum + rebuild(behind, 2, -1)
        forward_sign = jnp.where(slice_index == time_count - 1, -1.0, 1.0).astype(jnp.float32)
        backward_sign = jnp.where(slice_index == 0, -1.0, 1.0).astype(jnp.float32)
        ahead_time = project(spinor[after_index], 3, 1)
        hop_sum = hop_sum + rebuild(color_product(links_now[:, 3], ahead_time, False) * forward_sign, 3, 1)
        links_before = gauge_field[before_index][:, 3]
        behind_time = color_product(links_before, project(spinor[before_index], 3, -1), True) * backward_sign
        hop_sum = hop_sum + rebuild(behind_time, 3, -1)
        return (current.astype(jnp.float32) - HOPPING * hop_sum).astype(jnp.bfloat16)

    return lax.map(one_slice, jnp.arange(time_count, dtype=jnp.int32))


def reference(source, gauge_field):
    first_pass = apply_all(source, gauge_field)
    return apply_all(first_pass, gauge_field)
```

```python
import jax
import jax.numpy as jnp
from jax import lax
from jax.experimental import pallas as pl
from jax.experimental.pallas import tpu as pltpu
from jax.sharding import PartitionSpec as P

HOPPING = 0.124
F32 = jnp.float32
BF16 = jnp.bfloat16
LANES = 128


def lane_iota():
    return lax.broadcasted_iota(jnp.int32, (8, LANES), 1)


def row_iota():
    return lax.broadcasted_iota(jnp.int32, (8, LANES), 0)


def get(ref, k, r, j):
    return ref[k, r * 8 : r * 8 + 8, j * LANES : (j + 1) * LANES].astype(F32)


def links(u_ref, mu, j):
    def one(a, b, ri):
        row = ((mu * 3 + a) * 3 + b) * 2 + ri
        return jnp.broadcast_to(u_ref[row : row + 1, j * LANES : (j + 1) * LANES], (8, LANES))

    return [[(one(a, b, 0), one(a, b, 1)) for b in range(3)] for a in range(3)]


def times(u, h, adjoint):
    re, im = [], []
    for a in range(3):
        total_re = total_im = None
        for b in range(3):
            if adjoint:
                ur, ui = u[b][a]
                tr = ur * h[b] + ui * h[3 + b]
                ti = ur * h[3 + b] - ui * h[b]
            else:
                ur, ui = u[a][b]
                tr = ur * h[b] - ui * h[3 + b]
                ti = ur * h[3 + b] + ui * h[b]
            total_re = tr if total_re is None else total_re + tr
            total_im = ti if total_im is None else total_im + ti
        re.append(total_re)
        im.append(total_im)
    return re + im


def row_sign(r, value):
    if r == 0:
        return value
    if r == 2:
        return -value
    return jnp.where(row_iota() < 4, value, -value)


def swap_spins(tiles):
    turned = [pltpu.roll(t, 4, 0) for t in tiles]
    low = row_iota() < 4
    return [jnp.where(low, turned[(i + 1) % 3], turned[(i + 2) % 3]) for i in range(3)]


def mix(mu, r, up, dn, q):
    out = []
    for k in range(6):
        if mu in (0, 2):
            other = dn[k + 3] if k < 3 else dn[k - 3]
            other = other if k < 3 else -other
        else:
            other = -dn[k]
        if mu == 1:
            other = row_sign(r, -other)
        elif mu == 2:
            other = row_sign(r, other)
        out.append(up[k] + other if q > 0 else up[k] - other)
    return out


def spread(mu, r, k6, q):
    out = []
    for k in range(6):
        if mu in (0, 2):
            value = -k6[k + 3] if k < 3 else k6[k - 3]
        else:
            value = -k6[k]
        if mu == 1:
            value = row_sign(r, -value)
        elif mu == 2:
            value = row_sign(r, value)
        out.append(value if q > 0 else -value)
    return out


def shift_x(tile, ahead):
    x = lane_iota() & 15
    if ahead:
        return jnp.where(x == 15, pltpu.roll(tile, 15, 1), pltpu.roll(tile, 127, 1))
    return jnp.where(x == 0, pltpu.roll(tile, 113, 1), pltpu.roll(tile, 1, 1))


def shift_y(pair, ahead):
    lane = lane_iota()
    if ahead:
        a, b = (pltpu.roll(t, 112, 1) for t in pair)
        inside = lane < 112
    else:
        a, b = (pltpu.roll(t, 16, 1) for t in pair)
        inside = lane >= 16
    return [jnp.where(inside, a, b), jnp.where(inside, b, a)]


def project_edges(field, u_ref, flag_ref, z_one, z_two, t_near, t_far):
    odd = flag_ref[0] > 0.5
    for j in range(2):
        for mu, first, second in ((2, z_one, z_two), (3, t_near, t_far)):
            u = links(u_ref, mu, j)
            for r in range(3):
                up = [field(k, r, j) for k in range(6)]
                dn = [field(k, r + 3, j) for k in range(6)]
                fwd = mix(mu, r, up, dn, 1)
                bwd = times(u, mix(mu, r, up, dn, -1), True)
                if mu == 3:
                    fwd = [v * flag_ref[1] for v in fwd]
                    bwd = [v * flag_ref[2] for v in bwd]
                for k in range(6):
                    at = (k, slice(r * 8, r * 8 + 8), slice(j * LANES, (j + 1) * LANES))
                    first[at] = jnp.where(odd, fwd[k], bwd[k]).astype(BF16)
                    second[at] = jnp.where(odd, bwd[k], fwd[k]).astype(BF16)


def first_edges(flag_ref, f_ref, u_ref, z_one, z_two, t_near, t_far):
    project_edges(lambda k, r, j: get(f_ref, k, r, j), u_ref, flag_ref, z_one, z_two, t_near, t_far)


def space_hops(f_ref, u_ref, acc_ref):
    up_acc = {}
    dn_acc = {}

    def add(r, j, mu, k6, q):
        low = spread(mu, r, k6, q)
        for k in range(6):
            key = (k, r, j)
            up_acc[key] = k6[k] if key not in up_acc else up_acc[key] + k6[k]
            dn_acc[key] = low[k] if key not in dn_acc else dn_acc[key] + low[k]

    swapped = {}
    for j in range(2):
        for k in range(6):
            for r, tile in enumerate(swap_spins([get(f_ref, k, 3 + i, j) for i in range(3)])):
                swapped[k, r, j] = tile
    for r in range(3):
        up = [[get(f_ref, k, r, j) for k in range(6)] for j in range(2)]
        dn = [[swapped[k, r, j] for k in range(6)] for j in range(2)]
        for j in range(2):
            u = links(u_ref, 0, j)
            ahead = [shift_x(v, True) for v in mix(0, r, up[j], dn[j], 1)]
            add(r, j, 0, times(u, ahead, False), 1)
            behind = [shift_x(v, False) for v in times(u, mix(0, r, up[j], dn[j], -1), True)]
            add(r, j, 0, behind, -1)
        us = [links(u_ref, 1, j) for j in range(2)]
        half = [mix(1, r, up[j], dn[j], 1) for j in range(2)]
        moved = [shift_y([half[0][k], half[1][k]], True) for k in range(6)]
        for j in range(2):
            add(r, j, 1, times(us[j], [moved[k][j] for k in range(6)], False), 1)
        half = [times(us[j], mix(1, r, up[j], dn[j], -1), True) for j in range(2)]
        moved = [shift_y([half[0][k], half[1][k]], False) for k in range(6)]
        for j in range(2):
            add(r, j, 1, [moved[k][j] for k in range(6)], -1)
        for j in range(2):
            for k in range(6):
                lanes = slice(j * LANES, (j + 1) * LANES)
                acc_ref[k, r * 8 : r * 8 + 8, lanes] = up_acc.pop((k, r, j))
                acc_ref[k, 24 + r * 8 : 32 + r * 8, lanes] = dn_acc.pop((k, r, j))


def finish(flag_ref, f_ref, u_ref, acc_ref, z_one, z_two, t_near, t_far, out_ref):
    odd = flag_ref[0] > 0.5
    for j in range(2):
        lanes = slice(j * LANES, (j + 1) * LANES)
        uz = links(u_ref, 2, j)
        ut = links(u_ref, 3, j)
        low = [swap_spins([get(acc_ref, k, 3 + i, j) for i in range(3)]) for k in range(6)]
        for r in range(3):
            up = [get(acc_ref, k, r, j) for k in range(6)]
            dn = [low[k][r] for k in range(6)]
            one = [get(z_one, k, r, j) for k in range(6)]
            two = [get(z_two, k, r, j) for k in range(6)]
            near = [get(t_near, k, r, j) for k in range(6)]
            far = [get(t_far, k, r, j) for k in range(6)]
            parts = (
                (2, times(uz, [jnp.where(odd, a, b) for a, b in zip(one, two)], False), 1),
                (2, [jnp.where(odd, b, a) for a, b in zip(one, two)], -1),
                (3, times(ut, [jnp.where(odd, b, a) for a, b in zip(near, far)], False), 1),
                (3, [jnp.where(odd, a, b) for a, b in zip(near, far)], -1),
            )
            for mu, k6, q in parts:
                lower = spread(mu, r, k6, q)
                up = [a + b for a, b in zip(up, k6)]
                dn = [a + b for a, b in zip(dn, lower)]
            for k in range(6):
                for at, hop in ((r, up[k]), (r + 3, dn[k])):
                    value = get(f_ref, k, at, j) - HOPPING * hop
                    out_ref[k, at * 8 : at * 8 + 8, lanes] = value.astype(BF16)


def finish_and_edges(flag_ref, f_ref, u_ref, acc_ref, z1, z2, t1, t2, out_ref, z_one, z_two, t_near, t_far):
    finish(flag_ref, f_ref, u_ref, acc_ref, z1, z2, t1, t2, out_ref)
    project_edges(lambda k, r, j: get(out_ref, k, r, j), u_ref, flag_ref, z_one, z_two, t_near, t_far)


SPINOR = pltpu.VMEM((6, 48, 256), BF16)
HALF = pltpu.VMEM((6, 24, 256), BF16)
SUM = pltpu.VMEM((6, 48, 256), F32)


def call(kernel, name, outs, flags, *args):
    in_vmem = pl.BlockSpec(memory_space=pltpu.VMEM)
    specs = [in_vmem] * len(args)
    args = tuple(pltpu.with_memory_space_constraint(a, pltpu.VMEM) for a in args)
    given = args
    if flags is not None:
        specs = [pl.BlockSpec(memory_space=pltpu.SMEM)] + specs
        given = (flags,) + args
    return pl.pallas_call(
        kernel,
        out_shape=outs,
        in_specs=specs,
        out_specs=[in_vmem] * len(outs) if isinstance(outs, list) else in_vmem,
        name=name,
    )(*given)


def routes(nt, nz):
    z_one, z_two, t_near, t_far = [], [], [], []
    for t in range(nt):
        for z in range(nz):
            here = t * nz + z
            ahead, behind = t * nz + (z + 1) % nz, t * nz + (z - 1) % nz
            later, earlier = (t + 1) % nt * nz + z, (t - 1) % nt * nz + z
            odd = t % 2
            z_one.append((here, behind if odd else ahead))
            z_two.append((here, ahead if odd else behind))
            t_near.append((here, earlier if odd else later))
            t_far.append((here, later if odd else earlier))
    return z_one, z_two, t_near, t_far


def body(source, gauge_field):
    nt, nz = lax.axis_size("ta"), lax.axis_size("gz")
    ta = lax.axis_index("ta")
    flags = jnp.stack(
        [
            (ta % 2).astype(F32),
            jnp.where(ta == 0, -1.0, 1.0).astype(F32),
            jnp.where(ta == nt - 1, -1.0, 1.0).astype(F32),
        ]
    )
    field = source.reshape(2, 4, 3, 12, 256).transpose(0, 2, 1, 3, 4).reshape(6, 48, 256)
    u = gauge_field.reshape(4, 2, 3, 3, 256).transpose(0, 2, 3, 1, 4).reshape(72, 256).astype(F32)
    pairs = routes(nt, nz)

    def exchange(edges):
        return [lax.ppermute(e, ("ta", "gz"), p) for e, p in zip(edges, pairs)]

    edges = call(first_edges, "first_edges", [HALF] * 4, flags, field, u)
    halo = exchange(edges)
    acc = call(space_hops, "space_hops", SUM, None, field, u)
    field, *edges = call(finish_and_edges, "finish_and_edges", [SPINOR] + [HALF] * 4, flags, field, u, acc, *halo)
    halo = exchange(edges)
    acc = call(space_hops, "space_hops", SUM, None, field, u)
    field = call(finish, "finish", SPINOR, flags, field, u, acc, *halo)
    return field.reshape(2, 3, 4, 12, 256).transpose(0, 2, 1, 3, 4).reshape(source.shape)


def solution(mesh):
    spec = P("ta", "gz", None, None, None, None, None)
    return jax.shard_map(body, mesh=mesh, in_specs=(spec, spec), out_specs=spec, check_vma=False)
```

```python
import jax
import jax.numpy as jnp
from jax import lax
from jax.experimental import pallas as pl
from jax.experimental.pallas import tpu as pltpu
from jax.sharding import PartitionSpec as P

HOPPING = 0.124
F32 = jnp.float32
BF16 = jnp.bfloat16
LANES = 128


def lane_iota():
    return lax.broadcasted_iota(jnp.int32, (8, LANES), 1)


def row_iota():
    return lax.broadcasted_iota(jnp.int32, (8, LANES), 0)


def get(ref, k, r, j):
    return ref[k, r * 8 : r * 8 + 8, j * LANES : (j + 1) * LANES].astype(F32)


def links(u_ref, mu, j):
    def one(a, b, ri):
        row = ((mu * 3 + a) * 3 + b) * 2 + ri
        return jnp.broadcast_to(u_ref[row : row + 1, j * LANES : (j + 1) * LANES], (8, LANES))

    return [[(one(a, b, 0), one(a, b, 1)) for b in range(3)] for a in range(3)]


def times(u, h, adjoint):
    re, im = [], []
    for a in range(3):
        total_re = total_im = None
        for b in range(3):
            if adjoint:
                ur, ui = u[b][a]
                tr = ur * h[b] + ui * h[3 + b]
                ti = ur * h[3 + b] - ui * h[b]
            else:
                ur, ui = u[a][b]
                tr = ur * h[b] - ui * h[3 + b]
                ti = ur * h[3 + b] + ui * h[b]
            total_re = tr if total_re is None else total_re + tr
            total_im = ti if total_im is None else total_im + ti
        re.append(total_re)
        im.append(total_im)
    return re + im


def row_sign(r, value):
    if r == 0:
        return value
    if r == 2:
        return -value
    return jnp.where(row_iota() < 4, value, -value)


def swap_spins(tiles):
    turned = [pltpu.roll(t, 4, 0) for t in tiles]
    low = row_iota() < 4
    return [jnp.where(low, turned[(i + 1) % 3], turned[(i + 2) % 3]) for i in range(3)]


def mix(mu, r, up, dn, q):
    out = []
    for k in range(6):
        if mu in (0, 2):
            other = dn[k + 3] if k < 3 else dn[k - 3]
            other = other if k < 3 else -other
        else:
            other = -dn[k]
        if mu == 1:
            other = row_sign(r, -other)
        elif mu == 2:
            other = row_sign(r, other)
        out.append(up[k] + other if q > 0 else up[k] - other)
    return out


def spread(mu, r, k6, q):
    out = []
    for k in range(6):
        if mu in (0, 2):
            value = -k6[k + 3] if k < 3 else k6[k - 3]
        else:
            value = -k6[k]
        if mu == 1:
            value = row_sign(r, -value)
        elif mu == 2:
            value = row_sign(r, value)
        out.append(value if q > 0 else -value)
    return out


def shift_x(tile, ahead):
    x = lane_iota() & 15
    if ahead:
        return jnp.where(x == 15, pltpu.roll(tile, 15, 1), pltpu.roll(tile, 127, 1))
    return jnp.where(x == 0, pltpu.roll(tile, 113, 1), pltpu.roll(tile, 1, 1))


def shift_y(pair, ahead):
    lane = lane_iota()
    if ahead:
        a, b = (pltpu.roll(t, 112, 1) for t in pair)
        inside = lane < 112
    else:
        a, b = (pltpu.roll(t, 16, 1) for t in pair)
        inside = lane >= 16
    return [jnp.where(inside, a, b), jnp.where(inside, b, a)]


def project_edges(field, u_ref, z_one, z_two, t_far, t_near):
    ta = lax.axis_index("ta")
    turn_back = jnp.where(ta == 0, -1.0, 1.0).astype(F32)
    turn_on = jnp.where(ta == lax.axis_size("ta") - 1, -1.0, 1.0).astype(F32)
    odd = lax.axis_index("ta") % 2 == 1
    for j in range(2):
        for mu, first, second in ((2, z_one, z_two), (3, t_near, t_far)):
            u = links(u_ref, mu, j)
            for r in range(3):
                up = [field(k, r, j) for k in range(6)]
                dn = [field(k, r + 3, j) for k in range(6)]
                fwd = mix(mu, r, up, dn, 1)
                bwd = times(u, mix(mu, r, up, dn, -1), True)
                if mu == 3:
                    fwd = [v * turn_back for v in fwd]
                    bwd = [v * turn_on for v in bwd]
                for k in range(6):
                    at = (k, slice(r * 8, r * 8 + 8), slice(j * LANES, (j + 1) * LANES))
                    first[at] = jnp.where(odd, fwd[k], bwd[k]).astype(BF16)
                    second[at] = jnp.where(odd, bwd[k], fwd[k]).astype(BF16)


def first_edges(f_ref, u_ref, z_one, z_two, t_far, t_near):
    project_edges(lambda k, r, j: get(f_ref, k, r, j), u_ref, z_one, z_two, t_far, t_near)


def space_hops(f_ref, u_ref, acc_ref):
    up_acc = {}
    dn_acc = {}

    def add(r, j, mu, k6, q):
        low = spread(mu, r, k6, q)
        for k in range(6):
            key = (k, r, j)
            up_acc[key] = k6[k] if key not in up_acc else up_acc[key] + k6[k]
            dn_acc[key] = low[k] if key not in dn_acc else dn_acc[key] + low[k]

    swapped = {}
    for j in range(2):
        for k in range(6):
            for r, tile in enumerate(swap_spins([get(f_ref, k, 3 + i, j) for i in range(3)])):
                swapped[k, r, j] = tile
    for r in range(3):
        up = [[get(f_ref, k, r, j) for k in range(6)] for j in range(2)]
        dn = [[swapped[k, r, j] for k in range(6)] for j in range(2)]
        for j in range(2):
            u = links(u_ref, 0, j)
            ahead = [shift_x(v, True) for v in mix(0, r, up[j], dn[j], 1)]
            add(r, j, 0, times(u, ahead, False), 1)
            behind = [shift_x(v, False) for v in times(u, mix(0, r, up[j], dn[j], -1), True)]
            add(r, j, 0, behind, -1)
        us = [links(u_ref, 1, j) for j in range(2)]
        half = [mix(1, r, up[j], dn[j], 1) for j in range(2)]
        moved = [shift_y([half[0][k], half[1][k]], True) for k in range(6)]
        for j in range(2):
            add(r, j, 1, times(us[j], [moved[k][j] for k in range(6)], False), 1)
        half = [times(us[j], mix(1, r, up[j], dn[j], -1), True) for j in range(2)]
        moved = [shift_y([half[0][k], half[1][k]], False) for k in range(6)]
        for j in range(2):
            add(r, j, 1, [moved[k][j] for k in range(6)], -1)
        for j in range(2):
            for k in range(6):
                lanes = slice(j * LANES, (j + 1) * LANES)
                acc_ref[k, r * 8 : r * 8 + 8, lanes] = up_acc.pop((k, r, j))
                acc_ref[k, 24 + r * 8 : 32 + r * 8, lanes] = dn_acc.pop((k, r, j))


def finish(f_ref, u_ref, acc_ref, z_one, z_two, t_far, t_near, out_ref):
    odd = lax.axis_index("ta") % 2 == 1
    for j in range(2):
        lanes = slice(j * LANES, (j + 1) * LANES)
        uz = links(u_ref, 2, j)
        ut = links(u_ref, 3, j)
        low = [swap_spins([get(acc_ref, k, 3 + i, j) for i in range(3)]) for k in range(6)]
        for r in range(3):
            up = [get(acc_ref, k, r, j) for k in range(6)]
            dn = [low[k][r] for k in range(6)]
            one = [get(z_one, k, r, j) for k in range(6)]
            two = [get(z_two, k, r, j) for k in range(6)]
            near = [get(t_near, k, r, j) for k in range(6)]
            far = [get(t_far, k, r, j) for k in range(6)]
            parts = (
                (2, times(uz, [jnp.where(odd, a, b) for a, b in zip(one, two)], False), 1),
                (2, [jnp.where(odd, b, a) for a, b in zip(one, two)], -1),
                (3, times(ut, [jnp.where(odd, b, a) for a, b in zip(near, far)], False), 1),
                (3, [jnp.where(odd, a, b) for a, b in zip(near, far)], -1),
            )
            for mu, k6, q in parts:
                lower = spread(mu, r, k6, q)
                up = [a + b for a, b in zip(up, k6)]
                dn = [a + b for a, b in zip(dn, lower)]
            for k in range(6):
                for at, hop in ((r, up[k]), (r + 3, dn[k])):
                    value = get(f_ref, k, at, j) - HOPPING * hop
                    out_ref[k, at * 8 : at * 8 + 8, lanes] = value.astype(BF16)


def finish_and_edges(f_ref, u_ref, acc_ref, z1, z2, t1, t2, out_ref, z_one, z_two, t_far, t_near):
    finish(f_ref, u_ref, acc_ref, z1, z2, t1, t2, out_ref)
    project_edges(lambda k, r, j: get(out_ref, k, r, j), u_ref, z_one, z_two, t_far, t_near)


SPINOR = pltpu.VMEM((6, 48, 256), BF16)
HALF = pltpu.VMEM((6, 24, 256), BF16)
SUM = pltpu.VMEM((6, 48, 256), F32)


def call(kernel, name, outs, *args):
    in_vmem = pl.BlockSpec(memory_space=pltpu.VMEM)
    args = [pltpu.with_memory_space_constraint(a, pltpu.VMEM) for a in args]
    return pl.pallas_call(
        kernel,
        out_shape=outs,
        in_specs=[in_vmem] * len(args),
        out_specs=[in_vmem] * len(outs) if isinstance(outs, list) else in_vmem,
        name=name,
    )(*args)


def routes(nt, nz):
    z_one, z_two, t_far, t_near = [], [], [], []
    for t in range(nt):
        for z in range(nz):
            here = t * nz + z
            ahead, behind = t * nz + (z + 1) % nz, t * nz + (z - 1) % nz
            later, earlier = (t + 1) % nt * nz + z, (t - 1) % nt * nz + z
            odd = t % 2
            z_one.append((here, behind if odd else ahead))
            z_two.append((here, ahead if odd else behind))
            t_near.append((here, earlier if odd else later))
            t_far.append((here, later if odd else earlier))
    return z_one, z_two, t_far, t_near


def body(source, gauge_field):
    nt, nz = lax.axis_size("ta"), lax.axis_size("gz")
    field = source.reshape(2, 4, 3, 12, 256).transpose(0, 2, 1, 3, 4).reshape(6, 48, 256)
    u = gauge_field.reshape(4, 2, 3, 3, 256).transpose(0, 2, 3, 1, 4).reshape(72, 256).astype(F32)
    pairs = routes(nt, nz)

    def exchange(edges):
        return [lax.ppermute(e, ("ta", "gz"), p) for e, p in zip(edges, pairs)]

    edges = call(first_edges, "first_edges", [HALF] * 4, field, u)
    halo = exchange(edges)
    acc = call(space_hops, "space_hops", SUM, field, u)
    field, *edges = call(finish_and_edges, "finish_and_edges", [SPINOR] + [HALF] * 4, field, u, acc, *halo)
    halo = exchange(edges)
    acc = call(space_hops, "space_hops", SUM, field, u)
    field = call(finish, "finish", SPINOR, field, u, acc, *halo)
    return field.reshape(2, 3, 4, 12, 256).transpose(0, 2, 1, 3, 4).reshape(source.shape)


def solution(mesh):
    spec = P("ta", "gz", None, None, None, None, None)
    return jax.shard_map(body, mesh=mesh, in_specs=(spec, spec), out_specs=spec, check_vma=False)
```

```python
import jax
import jax.numpy as jnp
from jax import lax
from jax.experimental import pallas as pl
from jax.experimental.pallas import tpu as pltpu
from jax.sharding import PartitionSpec as P

HOPPING = 0.124
F32 = jnp.float32
BF16 = jnp.bfloat16
LANES = 128


def lane_iota():
    return lax.broadcasted_iota(jnp.int32, (8, LANES), 1)


def row_iota():
    return lax.broadcasted_iota(jnp.int32, (8, LANES), 0)


def get(ref, k, r, j):
    return ref[k, r * 8 : r * 8 + 8, j * LANES : (j + 1) * LANES].astype(F32)


def links(u_ref, mu, j):
    def one(a, b, ri):
        row = ((mu * 3 + a) * 3 + b) * 2 + ri
        return jnp.broadcast_to(u_ref[row : row + 1, j * LANES : (j + 1) * LANES], (8, LANES))

    return [[(one(a, b, 0), one(a, b, 1)) for b in range(3)] for a in range(3)]


def times(u, h, adjoint):
    re, im = [], []
    for a in range(3):
        total_re = total_im = None
        for b in range(3):
            if adjoint:
                ur, ui = u[b][a]
                tr = ur * h[b] + ui * h[3 + b]
                ti = ur * h[3 + b] - ui * h[b]
            else:
                ur, ui = u[a][b]
                tr = ur * h[b] - ui * h[3 + b]
                ti = ur * h[3 + b] + ui * h[b]
            total_re = tr if total_re is None else total_re + tr
            total_im = ti if total_im is None else total_im + ti
        re.append(total_re)
        im.append(total_im)
    return re + im


def row_sign(r, value):
    if r == 0:
        return value
    if r == 2:
        return -value
    return jnp.where(row_iota() < 4, value, -value)


def swap_spins(tiles):
    turned = [pltpu.roll(t, 4, 0) for t in tiles]
    low = row_iota() < 4
    return [jnp.where(low, turned[(i + 1) % 3], turned[(i + 2) % 3]) for i in range(3)]


def mix(mu, r, up, dn, q):
    out = []
    for k in range(6):
        if mu in (0, 2):
            other = dn[k + 3] if k < 3 else dn[k - 3]
            other = other if k < 3 else -other
        else:
            other = -dn[k]
        if mu == 1:
            other = row_sign(r, -other)
        elif mu == 2:
            other = row_sign(r, other)
        out.append(up[k] + other if q > 0 else up[k] - other)
    return out


def spread(mu, r, k6, q):
    out = []
    for k in range(6):
        if mu in (0, 2):
            value = -k6[k + 3] if k < 3 else k6[k - 3]
        else:
            value = -k6[k]
        if mu == 1:
            value = row_sign(r, -value)
        elif mu == 2:
            value = row_sign(r, value)
        out.append(value if q > 0 else -value)
    return out


def shift_x(tile, ahead):
    x = lane_iota() & 15
    if ahead:
        return jnp.where(x == 15, pltpu.roll(tile, 15, 1), pltpu.roll(tile, 127, 1))
    return jnp.where(x == 0, pltpu.roll(tile, 113, 1), pltpu.roll(tile, 1, 1))


def shift_y(pair, ahead):
    lane = lane_iota()
    if ahead:
        a, b = (pltpu.roll(t, 112, 1) for t in pair)
        inside = lane < 112
    else:
        a, b = (pltpu.roll(t, 16, 1) for t in pair)
        inside = lane >= 16
    return [jnp.where(inside, a, b), jnp.where(inside, b, a)]


def flips():
    ta = lax.axis_index("ta")
    return ta % 2 == 1, lax.axis_index("gz") % 2 == 1


def project_edges(field, u_ref, z_one, z_two, t_far, t_near):
    ta = lax.axis_index("ta")
    flip_t, flip_z = flips()
    turn_back = jnp.where(ta == 0, -1.0, 1.0).astype(F32)
    turn_on = jnp.where(ta == lax.axis_size("ta") - 1, -1.0, 1.0).astype(F32)
    for j in range(2):
        for mu, flip, first, second in ((2, flip_z, z_one, z_two), (3, flip_t, t_near, t_far)):
            u = links(u_ref, mu, j)
            for r in range(3):
                up = [field(k, r, j) for k in range(6)]
                dn = [field(k, r + 3, j) for k in range(6)]
                fwd = mix(mu, r, up, dn, 1)
                bwd = times(u, mix(mu, r, up, dn, -1), True)
                if mu == 3:
                    fwd = [v * turn_back for v in fwd]
                    bwd = [v * turn_on for v in bwd]
                for k in range(6):
                    at = (k, slice(r * 8, r * 8 + 8), slice(j * LANES, (j + 1) * LANES))
                    first[at] = jnp.where(flip, fwd[k], bwd[k]).astype(BF16)
                    second[at] = jnp.where(flip, bwd[k], fwd[k]).astype(BF16)


FIRST_ROUND = (0, 1, 2, 3)
SECOND_ROUND = (1, 0, 2, 3)


def in_place(order, items):
    return [items[order.index(i)] for i in range(4)]


def first_edges(f_ref, u_ref, *edges):
    project_edges(lambda k, r, j: get(f_ref, k, r, j), u_ref, *in_place(FIRST_ROUND, edges))


def space_hops(f_ref, u_ref, acc_ref):
    up_acc = {}
    dn_acc = {}

    def add(r, j, mu, k6, q):
        low = spread(mu, r, k6, q)
        for k in range(6):
            key = (k, r, j)
            up_acc[key] = k6[k] if key not in up_acc else up_acc[key] + k6[k]
            dn_acc[key] = low[k] if key not in dn_acc else dn_acc[key] + low[k]

    swapped = {}
    for j in range(2):
        for k in range(6):
            for r, tile in enumerate(swap_spins([get(f_ref, k, 3 + i, j) for i in range(3)])):
                swapped[k, r, j] = tile
    for r in range(3):
        up = [[get(f_ref, k, r, j) for k in range(6)] for j in range(2)]
        dn = [[swapped[k, r, j] for k in range(6)] for j in range(2)]
        for j in range(2):
            u = links(u_ref, 0, j)
            ahead = [shift_x(v, True) for v in mix(0, r, up[j], dn[j], 1)]
            add(r, j, 0, times(u, ahead, False), 1)
            behind = [shift_x(v, False) for v in times(u, mix(0, r, up[j], dn[j], -1), True)]
            add(r, j, 0, behind, -1)
        us = [links(u_ref, 1, j) for j in range(2)]
        half = [mix(1, r, up[j], dn[j], 1) for j in range(2)]
        moved = [shift_y([half[0][k], half[1][k]], True) for k in range(6)]
        for j in range(2):
            add(r, j, 1, times(us[j], [moved[k][j] for k in range(6)], False), 1)
        half = [times(us[j], mix(1, r, up[j], dn[j], -1), True) for j in range(2)]
        moved = [shift_y([half[0][k], half[1][k]], False) for k in range(6)]
        for j in range(2):
            add(r, j, 1, [moved[k][j] for k in range(6)], -1)
        for j in range(2):
            for k in range(6):
                lanes = slice(j * LANES, (j + 1) * LANES)
                acc_ref[k, r * 8 : r * 8 + 8, lanes] = up_acc.pop((k, r, j))
                acc_ref[k, 24 + r * 8 : 32 + r * 8, lanes] = dn_acc.pop((k, r, j))


def add_halo(f_ref, u_ref, acc_ref, z_one, z_two, t_far, t_near, out_ref):
    flip_t, flip_z = flips()
    for j in range(2):
        lanes = slice(j * LANES, (j + 1) * LANES)
        uz = links(u_ref, 2, j)
        ut = links(u_ref, 3, j)
        low = [swap_spins([get(acc_ref, k, 3 + i, j) for i in range(3)]) for k in range(6)]
        for r in range(3):
            up = [get(acc_ref, k, r, j) for k in range(6)]
            dn = [low[k][r] for k in range(6)]
            one = [get(z_one, k, r, j) for k in range(6)]
            two = [get(z_two, k, r, j) for k in range(6)]
            near = [get(t_near, k, r, j) for k in range(6)]
            far = [get(t_far, k, r, j) for k in range(6)]
            parts = (
                (2, times(uz, [jnp.where(flip_z, b, a) for a, b in zip(one, two)], False), 1),
                (2, [jnp.where(flip_z, a, b) for a, b in zip(one, two)], -1),
                (3, times(ut, [jnp.where(flip_t, b, a) for a, b in zip(near, far)], False), 1),
                (3, [jnp.where(flip_t, a, b) for a, b in zip(near, far)], -1),
            )
            for mu, k6, q in parts:
                lower = spread(mu, r, k6, q)
                up = [a + b for a, b in zip(up, k6)]
                dn = [a + b for a, b in zip(dn, lower)]
            for k in range(6):
                for at, hop in ((r, up[k]), (r + 3, dn[k])):
                    value = get(f_ref, k, at, j) - HOPPING * hop
                    out_ref[k, at * 8 : at * 8 + 8, lanes] = value.astype(BF16)


def finish_and_edges(f_ref, u_ref, acc_ref, h0, h1, h2, h3, out_ref, *edges):
    add_halo(f_ref, u_ref, acc_ref, *in_place(FIRST_ROUND, (h0, h1, h2, h3)), out_ref)
    project_edges(lambda k, r, j: get(out_ref, k, r, j), u_ref, *in_place(SECOND_ROUND, edges))


def finish(f_ref, u_ref, acc_ref, h0, h1, h2, h3, out_ref):
    add_halo(f_ref, u_ref, acc_ref, *in_place(SECOND_ROUND, (h0, h1, h2, h3)), out_ref)


SPINOR = pltpu.VMEM((6, 48, 256), BF16)
HALF = pltpu.VMEM((6, 24, 256), BF16)
SUM = pltpu.VMEM((6, 48, 256), F32)


def call(kernel, name, outs, *args):
    in_vmem = pl.BlockSpec(memory_space=pltpu.VMEM)
    args = [pltpu.with_memory_space_constraint(a, pltpu.VMEM) for a in args]
    return pl.pallas_call(
        kernel,
        out_shape=outs,
        in_specs=[in_vmem] * len(args),
        out_specs=[in_vmem] * len(outs) if isinstance(outs, list) else in_vmem,
        name=name,
    )(*args)


def routes(nt, nz):
    z_one, z_two, t_far, t_near = [], [], [], []
    for t in range(nt):
        for z in range(nz):
            here = t * nz + z
            ahead, behind = t * nz + (z + 1) % nz, t * nz + (z - 1) % nz
            later, earlier = (t + 1) % nt * nz + z, (t - 1) % nt * nz + z
            z_one.append((here, behind if z % 2 else ahead))
            z_two.append((here, ahead if z % 2 else behind))
            t_near.append((here, earlier if t % 2 else later))
            t_far.append((here, later if t % 2 else earlier))
    return z_one, z_two, t_far, t_near


def body(source, gauge_field):
    nt, nz = lax.axis_size("ta"), lax.axis_size("gz")
    field = source.reshape(2, 4, 3, 12, 256).transpose(0, 2, 1, 3, 4).reshape(6, 48, 256)
    u = gauge_field.reshape(4, 2, 3, 3, 256).transpose(0, 2, 3, 1, 4).reshape(72, 256).astype(F32)
    pairs = routes(nt, nz)

    def exchange(edges, order):
        return [lax.ppermute(e, ("ta", "gz"), pairs[i]) for i, e in zip(order, edges)]

    edges = call(first_edges, "first_edges", [HALF] * 4, field, u)
    halo = exchange(edges, FIRST_ROUND)
    acc = call(space_hops, "space_hops", SUM, field, u)
    field, *edges = call(finish_and_edges, "finish_and_edges", [SPINOR] + [HALF] * 4, field, u, acc, *halo)
    halo = exchange(edges, SECOND_ROUND)
    acc = call(space_hops, "space_hops", SUM, field, u)
    field = call(finish, "finish", SPINOR, field, u, acc, *halo)
    return field.reshape(2, 3, 4, 12, 256).transpose(0, 2, 1, 3, 4).reshape(source.shape)


def solution(mesh):
    spec = P("ta", "gz", None, None, None, None, None)
    return jax.shard_map(body, mesh=mesh, in_specs=(spec, spec), out_specs=spec, check_vma=False)
```

```python
import jax
import jax.numpy as jnp
from jax import lax
from jax.experimental import pallas as pl
from jax.experimental.pallas import tpu as pltpu
from jax.sharding import PartitionSpec as P

HOPPING = 0.124
F32 = jnp.float32
BF16 = jnp.bfloat16
LANES = 128


def lane_iota():
    return lax.broadcasted_iota(jnp.int32, (8, LANES), 1)


def row_iota():
    return lax.broadcasted_iota(jnp.int32, (8, LANES), 0)


def get(ref, k, r, j):
    return ref[k, r * 8 : r * 8 + 8, j * LANES : (j + 1) * LANES].astype(F32)


def links(u_ref, mu, j):
    def one(a, b, ri):
        row = ((mu * 3 + a) * 3 + b) * 2 + ri
        return jnp.broadcast_to(u_ref[row : row + 1, j * LANES : (j + 1) * LANES], (8, LANES))

    return [[(one(a, b, 0), one(a, b, 1)) for b in range(3)] for a in range(3)]


def times(u, h, adjoint):
    re, im = [], []
    for a in range(3):
        total_re = total_im = None
        for b in range(3):
            if adjoint:
                ur, ui = u[b][a]
                tr = ur * h[b] + ui * h[3 + b]
                ti = ur * h[3 + b] - ui * h[b]
            else:
                ur, ui = u[a][b]
                tr = ur * h[b] - ui * h[3 + b]
                ti = ur * h[3 + b] + ui * h[b]
            total_re = tr if total_re is None else total_re + tr
            total_im = ti if total_im is None else total_im + ti
        re.append(total_re)
        im.append(total_im)
    return re + im


def row_sign(r, value):
    if r == 0:
        return value
    if r == 2:
        return -value
    return jnp.where(row_iota() < 4, value, -value)


def swap_spins(tiles):
    turned = [pltpu.roll(t, 4, 0) for t in tiles]
    low = row_iota() < 4
    return [jnp.where(low, turned[(i + 1) % 3], turned[(i + 2) % 3]) for i in range(3)]


def mix(mu, r, up, dn, q):
    out = []
    for k in range(6):
        if mu in (0, 2):
            other = dn[k + 3] if k < 3 else dn[k - 3]
            other = other if k < 3 else -other
        else:
            other = -dn[k]
        if mu == 1:
            other = row_sign(r, -other)
        elif mu == 2:
            other = row_sign(r, other)
        out.append(up[k] + other if q > 0 else up[k] - other)
    return out


def spread(mu, r, k6, q):
    out = []
    for k in range(6):
        if mu in (0, 2):
            value = -k6[k + 3] if k < 3 else k6[k - 3]
        else:
            value = -k6[k]
        if mu == 1:
            value = row_sign(r, -value)
        elif mu == 2:
            value = row_sign(r, value)
        out.append(value if q > 0 else -value)
    return out


def shift_x(tile, ahead):
    x = lane_iota() & 15
    if ahead:
        return jnp.where(x == 15, pltpu.roll(tile, 15, 1), pltpu.roll(tile, 127, 1))
    return jnp.where(x == 0, pltpu.roll(tile, 113, 1), pltpu.roll(tile, 1, 1))


def shift_y(pair, ahead):
    lane = lane_iota()
    if ahead:
        a, b = (pltpu.roll(t, 112, 1) for t in pair)
        inside = lane < 112
    else:
        a, b = (pltpu.roll(t, 16, 1) for t in pair)
        inside = lane >= 16
    return [jnp.where(inside, a, b), jnp.where(inside, b, a)]


def flips(mixed):
    ta, gz = lax.axis_index("ta"), lax.axis_index("gz")
    return ta % 2 == 1, ((ta + gz) if mixed else gz) % 2 == 1


def project_edges(field, u_ref, mixed, z_one, z_two, t_far, t_near):
    ta = lax.axis_index("ta")
    flip_t, flip_z = flips(mixed)
    turn_back = jnp.where(ta == 0, -1.0, 1.0).astype(F32)
    turn_on = jnp.where(ta == lax.axis_size("ta") - 1, -1.0, 1.0).astype(F32)
    for j in range(2):
        for mu, flip, first, second in ((2, flip_z, z_one, z_two), (3, flip_t, t_near, t_far)):
            u = links(u_ref, mu, j)
            for r in range(3):
                up = [field(k, r, j) for k in range(6)]
                dn = [field(k, r + 3, j) for k in range(6)]
                fwd = mix(mu, r, up, dn, 1)
                bwd = times(u, mix(mu, r, up, dn, -1), True)
                if mu == 3:
                    fwd = [v * turn_back for v in fwd]
                    bwd = [v * turn_on for v in bwd]
                for k in range(6):
                    at = (k, slice(r * 8, r * 8 + 8), slice(j * LANES, (j + 1) * LANES))
                    first[at] = jnp.where(flip, fwd[k], bwd[k]).astype(BF16)
                    second[at] = jnp.where(flip, bwd[k], fwd[k]).astype(BF16)


FIRST_ROUND, FIRST_MIXED = (1, 0, 2, 3), True
SECOND_ROUND, SECOND_MIXED = (1, 0, 2, 3), False


def in_place(order, items):
    return [items[order.index(i)] for i in range(4)]


def first_edges(f_ref, u_ref, *edges):
    project_edges(lambda k, r, j: get(f_ref, k, r, j), u_ref, FIRST_MIXED, *in_place(FIRST_ROUND, edges))


def space_hops(f_ref, u_ref, acc_ref):
    up_acc = {}
    dn_acc = {}

    def add(r, j, mu, k6, q):
        low = spread(mu, r, k6, q)
        for k in range(6):
            key = (k, r, j)
            up_acc[key] = k6[k] if key not in up_acc else up_acc[key] + k6[k]
            dn_acc[key] = low[k] if key not in dn_acc else dn_acc[key] + low[k]

    swapped = {}
    for j in range(2):
        for k in range(6):
            for r, tile in enumerate(swap_spins([get(f_ref, k, 3 + i, j) for i in range(3)])):
                swapped[k, r, j] = tile
    for r in range(3):
        up = [[get(f_ref, k, r, j) for k in range(6)] for j in range(2)]
        dn = [[swapped[k, r, j] for k in range(6)] for j in range(2)]
        for j in range(2):
            u = links(u_ref, 0, j)
            ahead = [shift_x(v, True) for v in mix(0, r, up[j], dn[j], 1)]
            add(r, j, 0, times(u, ahead, False), 1)
            behind = [shift_x(v, False) for v in times(u, mix(0, r, up[j], dn[j], -1), True)]
            add(r, j, 0, behind, -1)
        us = [links(u_ref, 1, j) for j in range(2)]
        half = [mix(1, r, up[j], dn[j], 1) for j in range(2)]
        moved = [shift_y([half[0][k], half[1][k]], True) for k in range(6)]
        for j in range(2):
            add(r, j, 1, times(us[j], [moved[k][j] for k in range(6)], False), 1)
        half = [times(us[j], mix(1, r, up[j], dn[j], -1), True) for j in range(2)]
        moved = [shift_y([half[0][k], half[1][k]], False) for k in range(6)]
        for j in range(2):
            add(r, j, 1, [moved[k][j] for k in range(6)], -1)
        for j in range(2):
            for k in range(6):
                lanes = slice(j * LANES, (j + 1) * LANES)
                acc_ref[k, r * 8 : r * 8 + 8, lanes] = up_acc.pop((k, r, j))
                acc_ref[k, 24 + r * 8 : 32 + r * 8, lanes] = dn_acc.pop((k, r, j))


def add_halo(f_ref, u_ref, acc_ref, mixed, z_one, z_two, t_far, t_near, out_ref):
    flip_t, flip_z = flips(mixed)
    for j in range(2):
        lanes = slice(j * LANES, (j + 1) * LANES)
        uz = links(u_ref, 2, j)
        ut = links(u_ref, 3, j)
        low = [swap_spins([get(acc_ref, k, 3 + i, j) for i in range(3)]) for k in range(6)]
        for r in range(3):
            up = [get(acc_ref, k, r, j) for k in range(6)]
            dn = [low[k][r] for k in range(6)]
            one = [get(z_one, k, r, j) for k in range(6)]
            two = [get(z_two, k, r, j) for k in range(6)]
            near = [get(t_near, k, r, j) for k in range(6)]
            far = [get(t_far, k, r, j) for k in range(6)]
            parts = (
                (2, times(uz, [jnp.where(flip_z, b, a) for a, b in zip(one, two)], False), 1),
                (2, [jnp.where(flip_z, a, b) for a, b in zip(one, two)], -1),
                (3, times(ut, [jnp.where(flip_t, b, a) for a, b in zip(near, far)], False), 1),
                (3, [jnp.where(flip_t, a, b) for a, b in zip(near, far)], -1),
            )
            for mu, k6, q in parts:
                lower = spread(mu, r, k6, q)
                up = [a + b for a, b in zip(up, k6)]
                dn = [a + b for a, b in zip(dn, lower)]
            for k in range(6):
                for at, hop in ((r, up[k]), (r + 3, dn[k])):
                    value = get(f_ref, k, at, j) - HOPPING * hop
                    out_ref[k, at * 8 : at * 8 + 8, lanes] = value.astype(BF16)


def finish_and_edges(f_ref, u_ref, acc_ref, h0, h1, h2, h3, out_ref, *edges):
    add_halo(f_ref, u_ref, acc_ref, FIRST_MIXED, *in_place(FIRST_ROUND, (h0, h1, h2, h3)), out_ref)
    project_edges(lambda k, r, j: get(out_ref, k, r, j), u_ref, SECOND_MIXED, *in_place(SECOND_ROUND, edges))


def finish(f_ref, u_ref, acc_ref, h0, h1, h2, h3, out_ref):
    add_halo(f_ref, u_ref, acc_ref, SECOND_MIXED, *in_place(SECOND_ROUND, (h0, h1, h2, h3)), out_ref)


SPINOR = pltpu.VMEM((6, 48, 256), BF16)
HALF = pltpu.VMEM((6, 24, 256), BF16)
SUM = pltpu.VMEM((6, 48, 256), F32)


def call(kernel, name, outs, *args):
    in_vmem = pl.BlockSpec(memory_space=pltpu.VMEM)
    args = [pltpu.with_memory_space_constraint(a, pltpu.VMEM) for a in args]
    return pl.pallas_call(
        kernel,
        out_shape=outs,
        in_specs=[in_vmem] * len(args),
        out_specs=[in_vmem] * len(outs) if isinstance(outs, list) else in_vmem,
        name=name,
    )(*args)


def routes(nt, nz, mixed):
    z_one, z_two, t_far, t_near = [], [], [], []
    for t in range(nt):
        for z in range(nz):
            here = t * nz + z
            ahead, behind = t * nz + (z + 1) % nz, t * nz + (z - 1) % nz
            later, earlier = (t + 1) % nt * nz + z, (t - 1) % nt * nz + z
            flip = ((t + z) if mixed else z) % 2
            z_one.append((here, behind if flip else ahead))
            z_two.append((here, ahead if flip else behind))
            t_near.append((here, earlier if t % 2 else later))
            t_far.append((here, later if t % 2 else earlier))
    return z_one, z_two, t_far, t_near


def body(source, gauge_field):
    nt, nz = lax.axis_size("ta"), lax.axis_size("gz")
    field = source.reshape(2, 4, 3, 12, 256).transpose(0, 2, 1, 3, 4).reshape(6, 48, 256)
    u = gauge_field.reshape(4, 2, 3, 3, 256).transpose(0, 2, 3, 1, 4).reshape(72, 256).astype(F32)

    def exchange(edges, order, mixed):
        pairs = routes(nt, nz, mixed)
        return [lax.ppermute(e, ("ta", "gz"), pairs[i]) for i, e in zip(order, edges)]

    edges = call(first_edges, "first_edges", [HALF] * 4, field, u)
    halo = exchange(edges, FIRST_ROUND, FIRST_MIXED)
    acc = call(space_hops, "space_hops", SUM, field, u)
    field, *edges = call(finish_and_edges, "finish_and_edges", [SPINOR] + [HALF] * 4, field, u, acc, *halo)
    halo = exchange(edges, SECOND_ROUND, SECOND_MIXED)
    acc = call(space_hops, "space_hops", SUM, field, u)
    field = call(finish, "finish", SPINOR, field, u, acc, *halo)
    return field.reshape(2, 3, 4, 12, 256).transpose(0, 2, 1, 3, 4).reshape(source.shape)


def solution(mesh):
    spec = P("ta", "gz", None, None, None, None, None)
    return jax.shard_map(body, mesh=mesh, in_specs=(spec, spec), out_specs=spec, check_vma=False)
```

```python
import functools

import jax
import jax.numpy as jnp
from jax import lax
from jax.experimental import pallas as pl
from jax.experimental.pallas import tpu as pltpu
from jax.sharding import PartitionSpec as P

HOPPING = 0.124
F32 = jnp.float32
BF16 = jnp.bfloat16
LANES = 128


def lane_iota():
    return lax.broadcasted_iota(jnp.int32, (8, LANES), 1)


def row_iota():
    return lax.broadcasted_iota(jnp.int32, (8, LANES), 0)


def get(ref, k, r, j):
    return ref[k, r * 8 : r * 8 + 8, j * LANES : (j + 1) * LANES].astype(F32)


def links(u_ref, mu, j):
    def one(a, b, ri):
        row = ((mu * 3 + a) * 3 + b) * 2 + ri
        return jnp.broadcast_to(u_ref[row : row + 1, j * LANES : (j + 1) * LANES], (8, LANES))

    return [[(one(a, b, 0), one(a, b, 1)) for b in range(3)] for a in range(3)]


def times(u, h, adjoint):
    re, im = [], []
    for a in range(3):
        total_re = total_im = None
        for b in range(3):
            if adjoint:
                ur, ui = u[b][a]
                tr = ur * h[b] + ui * h[3 + b]
                ti = ur * h[3 + b] - ui * h[b]
            else:
                ur, ui = u[a][b]
                tr = ur * h[b] - ui * h[3 + b]
                ti = ur * h[3 + b] + ui * h[b]
            total_re = tr if total_re is None else total_re + tr
            total_im = ti if total_im is None else total_im + ti
        re.append(total_re)
        im.append(total_im)
    return re + im


def row_sign(r, value):
    if r == 0:
        return value
    if r == 2:
        return -value
    return jnp.where(row_iota() < 4, value, -value)


def swap_spins(tiles):
    turned = [pltpu.roll(t, 4, 0) for t in tiles]
    low = row_iota() < 4
    return [jnp.where(low, turned[(i + 1) % 3], turned[(i + 2) % 3]) for i in range(3)]


def mix(mu, r, up, dn, q):
    out = []
    for k in range(6):
        if mu in (0, 2):
            other = dn[k + 3] if k < 3 else dn[k - 3]
            other = other if k < 3 else -other
        else:
            other = -dn[k]
        if mu == 1:
            other = row_sign(r, -other)
        elif mu == 2:
            other = row_sign(r, other)
        out.append(up[k] + other if q > 0 else up[k] - other)
    return out


def spread(mu, r, k6, q):
    out = []
    for k in range(6):
        if mu in (0, 2):
            value = -k6[k + 3] if k < 3 else k6[k - 3]
        else:
            value = -k6[k]
        if mu == 1:
            value = row_sign(r, -value)
        elif mu == 2:
            value = row_sign(r, value)
        out.append(value if q > 0 else -value)
    return out


def shift_x(tile, ahead):
    x = lane_iota() & 15
    if ahead:
        return jnp.where(x == 15, pltpu.roll(tile, 15, 1), pltpu.roll(tile, 127, 1))
    return jnp.where(x == 0, pltpu.roll(tile, 113, 1), pltpu.roll(tile, 1, 1))


def shift_y(pair, ahead):
    lane = lane_iota()
    if ahead:
        a, b = (pltpu.roll(t, 112, 1) for t in pair)
        inside = lane < 112
    else:
        a, b = (pltpu.roll(t, 16, 1) for t in pair)
        inside = lane >= 16
    return [jnp.where(inside, a, b), jnp.where(inside, b, a)]


def flips(mixed):
    ta, gz = lax.axis_index("ta"), lax.axis_index("gz")
    return ta % 2 == 1, ((ta + gz) if mixed else gz) % 2 == 1


def project_edges(field, u_ref, mixed, z_one, z_two, t_far, t_near):
    ta = lax.axis_index("ta")
    flip_t, flip_z = flips(mixed)
    turn_back = jnp.where(ta == 0, -1.0, 1.0).astype(F32)
    turn_on = jnp.where(ta == lax.axis_size("ta") - 1, -1.0, 1.0).astype(F32)
    for j in range(2):
        for mu, flip, first, second in ((2, flip_z, z_one, z_two), (3, flip_t, t_near, t_far)):
            u = links(u_ref, mu, j)
            for r in range(3):
                up = [field(k, r, j) for k in range(6)]
                dn = [field(k, r + 3, j) for k in range(6)]
                fwd = mix(mu, r, up, dn, 1)
                bwd = times(u, mix(mu, r, up, dn, -1), True)
                if mu == 3:
                    fwd = [v * turn_back for v in fwd]
                    bwd = [v * turn_on for v in bwd]
                for k in range(6):
                    at = (k, slice(r * 8, r * 8 + 8), slice(j * LANES, (j + 1) * LANES))
                    first[at] = jnp.where(flip, fwd[k], bwd[k]).astype(BF16)
                    second[at] = jnp.where(flip, bwd[k], fwd[k]).astype(BF16)


FIRST_ROUND, FIRST_MIXED = (1, 0, 2, 3), True
SECOND_ROUND, SECOND_MIXED = (1, 0, 2, 3), False


def in_place(order, items):
    return [items[order.index(i)] for i in range(4)]


def space_hops(f_ref, u_ref, acc_ref):
    up_acc = {}
    dn_acc = {}

    def add(r, j, mu, k6, q):
        low = spread(mu, r, k6, q)
        for k in range(6):
            key = (k, r, j)
            up_acc[key] = k6[k] if key not in up_acc else up_acc[key] + k6[k]
            dn_acc[key] = low[k] if key not in dn_acc else dn_acc[key] + low[k]

    swapped = {}
    for j in range(2):
        for k in range(6):
            for r, tile in enumerate(swap_spins([get(f_ref, k, 3 + i, j) for i in range(3)])):
                swapped[k, r, j] = tile
    for r in range(3):
        up = [[get(f_ref, k, r, j) for k in range(6)] for j in range(2)]
        dn = [[swapped[k, r, j] for k in range(6)] for j in range(2)]
        for j in range(2):
            u = links(u_ref, 0, j)
            ahead = [shift_x(v, True) for v in mix(0, r, up[j], dn[j], 1)]
            add(r, j, 0, times(u, ahead, False), 1)
            behind = [shift_x(v, False) for v in times(u, mix(0, r, up[j], dn[j], -1), True)]
            add(r, j, 0, behind, -1)
        us = [links(u_ref, 1, j) for j in range(2)]
        half = [mix(1, r, up[j], dn[j], 1) for j in range(2)]
        moved = [shift_y([half[0][k], half[1][k]], True) for k in range(6)]
        for j in range(2):
            add(r, j, 1, times(us[j], [moved[k][j] for k in range(6)], False), 1)
        half = [times(us[j], mix(1, r, up[j], dn[j], -1), True) for j in range(2)]
        moved = [shift_y([half[0][k], half[1][k]], False) for k in range(6)]
        for j in range(2):
            add(r, j, 1, [moved[k][j] for k in range(6)], -1)
        for j in range(2):
            for k in range(6):
                lanes = slice(j * LANES, (j + 1) * LANES)
                acc_ref[k, r * 8 : r * 8 + 8, lanes] = up_acc.pop((k, r, j))
                acc_ref[k, 24 + r * 8 : 32 + r * 8, lanes] = dn_acc.pop((k, r, j))


def accumulate(mu, r, k6, q, up, dn):
    lower = spread(mu, r, k6, q)
    return [a + b for a, b in zip(up, k6)], [a + b for a, b in zip(dn, lower)]


def add_z(order, mixed, f_ref, u_ref, acc_ref, h0, h1, base_ref):
    _, flip_z = flips(mixed)
    z_one, z_two = (h0, h1) if order.index(0) < order.index(1) else (h1, h0)
    for j in range(2):
        lanes = slice(j * LANES, (j + 1) * LANES)
        uz = links(u_ref, 2, j)
        low = [swap_spins([get(acc_ref, k, 3 + i, j) for i in range(3)]) for k in range(6)]
        for r in range(3):
            up = [get(acc_ref, k, r, j) for k in range(6)]
            dn = [low[k][r] for k in range(6)]
            one = [get(z_one, k, r, j) for k in range(6)]
            two = [get(z_two, k, r, j) for k in range(6)]
            ahead = times(uz, [jnp.where(flip_z, b, a) for a, b in zip(one, two)], False)
            behind = [jnp.where(flip_z, a, b) for a, b in zip(one, two)]
            up, dn = accumulate(2, r, ahead, 1, up, dn)
            up, dn = accumulate(2, r, behind, -1, up, dn)
            for k in range(6):
                for at, hop in ((r, up[k]), (r + 3, dn[k])):
                    base_ref[k, at * 8 : at * 8 + 8, lanes] = get(f_ref, k, at, j) - HOPPING * hop


def add_t(u_ref, base_ref, t_far, t_near, out_ref):
    flip_t, _ = flips(False)
    for j in range(2):
        lanes = slice(j * LANES, (j + 1) * LANES)
        ut = links(u_ref, 3, j)
        for r in range(3):
            near = [get(t_near, k, r, j) for k in range(6)]
            far = [get(t_far, k, r, j) for k in range(6)]
            up = times(ut, [jnp.where(flip_t, b, a) for a, b in zip(near, far)], False)
            dn = spread(3, r, up, 1)
            up, dn = accumulate(3, r, [jnp.where(flip_t, a, b) for a, b in zip(near, far)], -1, up, dn)
            for k in range(6):
                for at, hop in ((r, up[k]), (r + 3, dn[k])):
                    value = get(base_ref, k, at, j) - HOPPING * hop
                    out_ref[k, at * 8 : at * 8 + 8, lanes] = value.astype(BF16)


def first_edges(f_ref, u_ref, *edges):
    project_edges(lambda k, r, j: get(f_ref, k, r, j), u_ref, FIRST_MIXED, *in_place(FIRST_ROUND, edges))


def add_t_and_edges(u_ref, base_ref, t_far, t_near, out_ref, *edges):
    add_t(u_ref, base_ref, t_far, t_near, out_ref)
    project_edges(lambda k, r, j: get(out_ref, k, r, j), u_ref, SECOND_MIXED, *in_place(SECOND_ROUND, edges))


SPINOR = pltpu.VMEM((6, 48, 256), BF16)
HALF = pltpu.VMEM((6, 24, 256), BF16)
SUM = pltpu.VMEM((6, 48, 256), F32)


def call(kernel, name, outs, *args):
    in_vmem = pl.BlockSpec(memory_space=pltpu.VMEM)
    args = [pltpu.with_memory_space_constraint(a, pltpu.VMEM) for a in args]
    return pl.pallas_call(
        kernel,
        out_shape=outs,
        in_specs=[in_vmem] * len(args),
        out_specs=[in_vmem] * len(outs) if isinstance(outs, list) else in_vmem,
        name=name,
    )(*args)


def routes(nt, nz, mixed):
    z_one, z_two, t_far, t_near = [], [], [], []
    for t in range(nt):
        for z in range(nz):
            here = t * nz + z
            ahead, behind = t * nz + (z + 1) % nz, t * nz + (z - 1) % nz
            later, earlier = (t + 1) % nt * nz + z, (t - 1) % nt * nz + z
            flip = ((t + z) if mixed else z) % 2
            z_one.append((here, behind if flip else ahead))
            z_two.append((here, ahead if flip else behind))
            t_near.append((here, earlier if t % 2 else later))
            t_far.append((here, later if t % 2 else earlier))
    return z_one, z_two, t_far, t_near


def body(source, gauge_field):
    nt, nz = lax.axis_size("ta"), lax.axis_size("gz")
    field = source.reshape(2, 4, 3, 12, 256).transpose(0, 2, 1, 3, 4).reshape(6, 48, 256)
    u = gauge_field.reshape(4, 2, 3, 3, 256).transpose(0, 2, 3, 1, 4).reshape(72, 256).astype(F32)

    def exchange(edges, order, mixed):
        pairs = routes(nt, nz, mixed)
        return [lax.ppermute(e, ("ta", "gz"), pairs[i]) for i, e in zip(order, edges)]

    def hops(field, halo, order, mixed):
        acc = call(space_hops, "space_hops", SUM, field, u)
        z_halo = [h for i, h in zip(order, halo) if i < 2]
        base = call(functools.partial(add_z, order, mixed), "add_z", SUM, field, u, acc, *z_halo)
        _, _, t_far, t_near = in_place(order, halo)
        return u, base, t_far, t_near

    edges = call(first_edges, "first_edges", [HALF] * 4, field, u)
    halo = exchange(edges, FIRST_ROUND, FIRST_MIXED)
    args = hops(field, halo, FIRST_ROUND, FIRST_MIXED)
    field, *edges = call(add_t_and_edges, "add_t_and_edges", [SPINOR] + [HALF] * 4, *args)
    halo = exchange(edges, SECOND_ROUND, SECOND_MIXED)
    field = call(add_t, "add_t", SPINOR, *hops(field, halo, SECOND_ROUND, SECOND_MIXED))
    return field.reshape(2, 3, 4, 12, 256).transpose(0, 2, 1, 3, 4).reshape(source.shape)


def solution(mesh):
    spec = P("ta", "gz", None, None, None, None, None)
    return jax.shard_map(body, mesh=mesh, in_specs=(spec, spec), out_specs=spec, check_vma=False)
```

```python
import functools

import jax
import jax.numpy as jnp
from jax import lax
from jax.experimental import pallas as pl
from jax.experimental.pallas import tpu as pltpu
from jax.sharding import PartitionSpec as P

HOPPING = 0.124
F32 = jnp.float32
BF16 = jnp.bfloat16
LANES = 128


def lane_iota():
    return lax.broadcasted_iota(jnp.int32, (8, LANES), 1)


def row_iota():
    return lax.broadcasted_iota(jnp.int32, (8, LANES), 0)


def get(ref, k, r, j):
    return ref[k, r * 8 : r * 8 + 8, j * LANES : (j + 1) * LANES].astype(F32)


def links(u_ref, mu, j):
    def one(a, b, ri):
        row = ((mu * 3 + a) * 3 + b) * 2 + ri
        return jnp.broadcast_to(u_ref[row : row + 1, j * LANES : (j + 1) * LANES], (8, LANES))

    return [[(one(a, b, 0), one(a, b, 1)) for b in range(3)] for a in range(3)]


def times(u, h, adjoint):
    re, im = [], []
    for a in range(3):
        total_re = total_im = None
        for b in range(3):
            if adjoint:
                ur, ui = u[b][a]
                tr = ur * h[b] + ui * h[3 + b]
                ti = ur * h[3 + b] - ui * h[b]
            else:
                ur, ui = u[a][b]
                tr = ur * h[b] - ui * h[3 + b]
                ti = ur * h[3 + b] + ui * h[b]
            total_re = tr if total_re is None else total_re + tr
            total_im = ti if total_im is None else total_im + ti
        re.append(total_re)
        im.append(total_im)
    return re + im


def row_sign(r, value):
    if r == 0:
        return value
    if r == 2:
        return -value
    return jnp.where(row_iota() < 4, value, -value)


def swap_spins(tiles):
    turned = [pltpu.roll(t, 4, 0) for t in tiles]
    low = row_iota() < 4
    return [jnp.where(low, turned[(i + 1) % 3], turned[(i + 2) % 3]) for i in range(3)]


def mix(mu, r, up, dn, q):
    out = []
    for k in range(6):
        if mu in (0, 2):
            other = dn[k + 3] if k < 3 else dn[k - 3]
            other = other if k < 3 else -other
        else:
            other = -dn[k]
        if mu == 1:
            other = row_sign(r, -other)
        elif mu == 2:
            other = row_sign(r, other)
        out.append(up[k] + other if q > 0 else up[k] - other)
    return out


def spread(mu, r, k6, q):
    out = []
    for k in range(6):
        if mu in (0, 2):
            value = -k6[k + 3] if k < 3 else k6[k - 3]
        else:
            value = -k6[k]
        if mu == 1:
            value = row_sign(r, -value)
        elif mu == 2:
            value = row_sign(r, value)
        out.append(value if q > 0 else -value)
    return out


def shift_x(tile, ahead):
    x = lane_iota() & 15
    if ahead:
        return jnp.where(x == 15, pltpu.roll(tile, 15, 1), pltpu.roll(tile, 127, 1))
    return jnp.where(x == 0, pltpu.roll(tile, 113, 1), pltpu.roll(tile, 1, 1))


def shift_y(pair, ahead):
    lane = lane_iota()
    if ahead:
        a, b = (pltpu.roll(t, 112, 1) for t in pair)
        inside = lane < 112
    else:
        a, b = (pltpu.roll(t, 16, 1) for t in pair)
        inside = lane >= 16
    return [jnp.where(inside, a, b), jnp.where(inside, b, a)]


Z_AHEAD, Z_BEHIND, T_NEAR, T_FAR = range(4)
FIRST = ((2, 1, 3, 0), (1, 2, 3, 0), (2, 1, 0, 3), (1, 2, 0, 3), (1, 2, 3, 0), (2, 1, 3, 0), (1, 2, 3, 0), (2, 1, 3, 0))
SECOND = ((1, 0, 3, 2), (1, 2, 0, 3), (2, 3, 0, 1), (1, 2, 0, 3), (1, 2, 3, 0), (3, 1, 2, 0), (1, 2, 3, 0), (0, 2, 1, 3))


def arrivals(table):
    def row(p, z):
        other = 4 * (1 - p) + z
        return table[4 * p + (z + 1) % 4][Z_BEHIND], table[4 * p + (z - 1) % 4][Z_AHEAD], table[other][T_NEAR], table[other][T_FAR]

    return tuple(row(p, z) for p in range(2) for z in range(4))


def row_flags():
    row = 4 * (lax.axis_index("ta") % 2) + lax.axis_index("gz") % 4
    return [row == i for i in range(8)]


def pick(flags, which, tiles):
    kinds = sorted(set(which), key=which.count)
    out = tiles[kinds[-1]]
    for kind in kinds[:-1]:
        holds = functools.reduce(jnp.logical_or, [f for f, w in zip(flags, which) if w == kind])
        out = [jnp.where(holds, a, b) for a, b in zip(tiles[kind], out)]
    return out


def project_edges(field, u_ref, table, edges):
    ta = lax.axis_index("ta")
    flags = row_flags()
    flip = ta % 2 == 1
    turn_back = jnp.where(ta == 0, -1.0, 1.0).astype(F32)
    turn_on = jnp.where(ta == lax.axis_size("ta") - 1, -1.0, 1.0).astype(F32)
    for j in range(2):
        uz, ut = links(u_ref, 2, j), links(u_ref, 3, j)
        for r in range(3):
            up = [field(k, r, j) for k in range(6)]
            dn = [field(k, r + 3, j) for k in range(6)]
            z_fwd = mix(2, r, up, dn, 1)
            z_bwd = times(uz, mix(2, r, up, dn, -1), True)
            t_fwd = [v * turn_back for v in mix(3, r, up, dn, 1)]
            t_bwd = [v * turn_on for v in times(ut, mix(3, r, up, dn, -1), True)]
            near = [jnp.where(flip, a, b) for a, b in zip(t_fwd, t_bwd)]
            far = [jnp.where(flip, b, a) for a, b in zip(t_fwd, t_bwd)]
            for swap, ref in enumerate(edges):
                sent = pick(flags, [row.index(swap) for row in table], [z_bwd, z_fwd, near, far])
                for k in range(6):
                    ref[k, r * 8 : r * 8 + 8, j * LANES : (j + 1) * LANES] = sent[k].astype(BF16)


def received(flags, table, kind, refs, r, j):
    which = [row[kind] for row in arrivals(table)]
    tiles = {swap: [get(refs[swap], k, r, j) for k in range(6)] for swap in set(which)}
    return pick(flags, which, tiles)


def space_hops(f_ref, u_ref, acc_ref):
    up_acc = {}
    dn_acc = {}

    def add(r, j, mu, k6, q):
        low = spread(mu, r, k6, q)
        for k in range(6):
            key = (k, r, j)
            up_acc[key] = k6[k] if key not in up_acc else up_acc[key] + k6[k]
            dn_acc[key] = low[k] if key not in dn_acc else dn_acc[key] + low[k]

    swapped = {}
    for j in range(2):
        for k in range(6):
            for r, tile in enumerate(swap_spins([get(f_ref, k, 3 + i, j) for i in range(3)])):
                swapped[k, r, j] = tile
    for r in range(3):
        up = [[get(f_ref, k, r, j) for k in range(6)] for j in range(2)]
        dn = [[swapped[k, r, j] for k in range(6)] for j in range(2)]
        for j in range(2):
            u = links(u_ref, 0, j)
            ahead = [shift_x(v, True) for v in mix(0, r, up[j], dn[j], 1)]
            add(r, j, 0, times(u, ahead, False), 1)
            behind = [shift_x(v, False) for v in times(u, mix(0, r, up[j], dn[j], -1), True)]
            add(r, j, 0, behind, -1)
        us = [links(u_ref, 1, j) for j in range(2)]
        half = [mix(1, r, up[j], dn[j], 1) for j in range(2)]
        moved = [shift_y([half[0][k], half[1][k]], True) for k in range(6)]
        for j in range(2):
            add(r, j, 1, times(us[j], [moved[k][j] for k in range(6)], False), 1)
        half = [times(us[j], mix(1, r, up[j], dn[j], -1), True) for j in range(2)]
        moved = [shift_y([half[0][k], half[1][k]], False) for k in range(6)]
        for j in range(2):
            add(r, j, 1, [moved[k][j] for k in range(6)], -1)
        for j in range(2):
            for k in range(6):
                lanes = slice(j * LANES, (j + 1) * LANES)
                acc_ref[k, r * 8 : r * 8 + 8, lanes] = up_acc.pop((k, r, j))
                acc_ref[k, 24 + r * 8 : 32 + r * 8, lanes] = dn_acc.pop((k, r, j))


def accumulate(mu, r, k6, q, up, dn):
    lower = spread(mu, r, k6, q)
    return [a + b for a, b in zip(up, k6)], [a + b for a, b in zip(dn, lower)]


def swaps_of(table, *kinds):
    return sorted({row[kind] for row in arrivals(table) for kind in kinds})


def z_swaps(table):
    return list(range(max(swaps_of(table, Z_AHEAD, Z_BEHIND)) + 1))


def add_z(table, f_ref, u_ref, acc_ref, *refs):
    *halo, base_ref = refs
    halo = dict(zip(z_swaps(table), halo))
    flags = row_flags()
    for j in range(2):
        lanes = slice(j * LANES, (j + 1) * LANES)
        uz = links(u_ref, 2, j)
        low = [swap_spins([get(acc_ref, k, 3 + i, j) for i in range(3)]) for k in range(6)]
        for r in range(3):
            up = [get(acc_ref, k, r, j) for k in range(6)]
            dn = [low[k][r] for k in range(6)]
            ahead = times(uz, received(flags, table, Z_AHEAD, halo, r, j), False)
            up, dn = accumulate(2, r, ahead, 1, up, dn)
            up, dn = accumulate(2, r, received(flags, table, Z_BEHIND, halo, r, j), -1, up, dn)
            for k in range(6):
                for at, hop in ((r, up[k]), (r + 3, dn[k])):
                    base_ref[k, at * 8 : at * 8 + 8, lanes] = get(f_ref, k, at, j) - HOPPING * hop


def add_t(table, u_ref, base_ref, *refs):
    *halo, out_ref = refs
    halo = dict(zip(swaps_of(table, T_NEAR, T_FAR), halo))
    flags = row_flags()
    flip = lax.axis_index("ta") % 2 == 1
    for j in range(2):
        lanes = slice(j * LANES, (j + 1) * LANES)
        ut = links(u_ref, 3, j)
        for r in range(3):
            near = received(flags, table, T_NEAR, halo, r, j)
            far = received(flags, table, T_FAR, halo, r, j)
            up = times(ut, [jnp.where(flip, b, a) for a, b in zip(near, far)], False)
            dn = spread(3, r, up, 1)
            up, dn = accumulate(3, r, [jnp.where(flip, a, b) for a, b in zip(near, far)], -1, up, dn)
            for k in range(6):
                for at, hop in ((r, up[k]), (r + 3, dn[k])):
                    value = get(base_ref, k, at, j) - HOPPING * hop
                    out_ref[k, at * 8 : at * 8 + 8, lanes] = value.astype(BF16)


def first_edges(f_ref, u_ref, *edges):
    project_edges(lambda k, r, j: get(f_ref, k, r, j), u_ref, FIRST, edges)


def add_t_and_edges(u_ref, base_ref, *refs):
    count = len(swaps_of(FIRST, T_NEAR, T_FAR))
    out_ref = refs[count]
    add_t(FIRST, u_ref, base_ref, *refs[: count + 1])
    project_edges(lambda k, r, j: get(out_ref, k, r, j), u_ref, SECOND, refs[count + 1 :])


SPINOR = pltpu.VMEM((6, 48, 256), BF16)
HALF = pltpu.VMEM((6, 24, 256), BF16)
SUM = pltpu.VMEM((6, 48, 256), F32)


def call(kernel, name, outs, *args):
    in_vmem = pl.BlockSpec(memory_space=pltpu.VMEM)
    args = [pltpu.with_memory_space_constraint(a, pltpu.VMEM) for a in args]
    return pl.pallas_call(
        kernel,
        out_shape=outs,
        in_specs=[in_vmem] * len(args),
        out_specs=[in_vmem] * len(outs) if isinstance(outs, list) else in_vmem,
        name=name,
    )(*args)


def routes(nt, nz, table):
    out = [[], [], [], []]
    for t in range(nt):
        for z in range(nz):
            for kind, swap in enumerate(table[4 * (t % 2) + z % 4]):
                partner_z = z + 1 if kind == Z_AHEAD else z - 1 if kind == Z_BEHIND else z
                later = (kind == T_NEAR) == (t % 2 == 0)
                partner_t = t if kind in (Z_AHEAD, Z_BEHIND) else t + 1 if later else t - 1
                out[swap].append((t * nz + z, partner_t % nt * nz + partner_z % nz))
    return out


def body(source, gauge_field):
    nt, nz = lax.axis_size("ta"), lax.axis_size("gz")
    field = source.reshape(2, 4, 3, 12, 256).transpose(0, 2, 1, 3, 4).reshape(6, 48, 256)
    u = gauge_field.reshape(4, 2, 3, 3, 256).transpose(0, 2, 3, 1, 4).reshape(72, 256).astype(F32)

    def exchange(edges, table):
        return [lax.ppermute(e, ("ta", "gz"), p) for e, p in zip(edges, routes(nt, nz, table))]

    def hops(field, halo, table):
        acc = call(space_hops, "space_hops", SUM, field, u)
        z_halo = [halo[i] for i in z_swaps(table)]
        base = call(functools.partial(add_z, table), "add_z", SUM, field, u, acc, *z_halo)
        return u, base, *[halo[i] for i in swaps_of(table, T_NEAR, T_FAR)]

    halo = exchange(call(first_edges, "first_edges", [HALF] * 4, field, u), FIRST)
    field, *edges = call(add_t_and_edges, "add_t_and_edges", [SPINOR] + [HALF] * 4, *hops(field, halo, FIRST))
    halo = exchange(edges, SECOND)
    field = call(functools.partial(add_t, SECOND), "add_t", SPINOR, *hops(field, halo, SECOND))
    return field.reshape(2, 3, 4, 12, 256).transpose(0, 2, 1, 3, 4).reshape(source.shape)


def solution(mesh):
    spec = P("ta", "gz", None, None, None, None, None)
    return jax.shard_map(body, mesh=mesh, in_specs=(spec, spec), out_specs=spec, check_vma=False)
```
